32 devices in a mesh: seq: 4 (over z), tp: 4 (over y, core), roll: 2 (over x).
Axes of the slice: x: 2, y: 2, z: 4, core: 2. Of those that a mesh axis runs over, the one named last changes fastest.
Arguments:
- hidden: bfloat16 [8, 3584], P('roll'), may hold values from -6 to 6
- norm_gain: bfloat16 [3584], replicated, may hold values from 0.25 to 1.75
- qkv_bias: bfloat16 [3072], replicated, may hold values from -20 to 20
- qkv_weight: bfloat16 [3584, 3072], P(('seq', 'tp', 'roll')), may hold values from -0.09375 to 0.09375
- out_weight: bfloat16 [3584, 2048], P(('seq', 'tp', 'roll')), may hold values from -0.125 to 0.125
- key_cache: bfloat16 [8, 16384, 512], P('roll', ('seq', 'tp')), may hold values from -16 to 16
- value_cache: bfloat16 [8, 16384, 512], P('roll', ('seq', 'tp')), may hold values from -16 to 16
- cache_len: int32 [8], P('roll'), may hold values from 8192 to 16384, as said below
- block_pos: int32 [8, 32], P('roll', ('seq', 'tp')), may hold values from 0 to 16383, as said below
Outputs:
- attended: bfloat16 [8, 3584], P('roll')
- fresh_kv: bfloat16 [8, 1024], P('roll')
- served_qkv: bfloat16 [3584, 3072], P(None, 'tp')
- served_out: bfloat16 [3584, 2048], P(None, 'tp')
The draws below stay inside these ranges and needn't reach their ends.
Inputs may be any that keep to these rules, and one draw needn't show every extreme that they name: `cache_len`: in every draw one rollout has all 16384 positions cached. With i = cache_len[r] mod 8192, and c the 8192-position stretch that holds position cache_len[r]: block_pos[r, b] is i where block b lies in c, i + 8192 where it lies in a later stretch or in the stretch just before c, and 16383 elsewhere.
All inputs are finite; a program needn't handle non-finite values.
Results may differ from the reference program's by a relative error of at most 0.009.
Values may be sent and summed in bfloat16 or wider, within the bound.
A program may use at most 128 MiB of HBM per device.

```python
import jax
import jax.numpy as jnp
import numpy as np
from jax import lax

D = 3584
HQ = 16
KVH = 4
HD = 128
QKV = 3072
SCOLS = 768
ROLLS = 8
LEN = 16384
BLOCK = 512
NBLK = 32
STRETCH = 8192
N_TP = 4


def shared_lengths(key):
    base_draw = jax.random.randint(jax.random.fold_in(key, 11), (ROLLS,), LEN // 2, LEN + 1)
    chosen = jax.random.randint(jax.random.fold_in(key, 12), (), 0, ROLLS)
    return jnp.where(jnp.arange(ROLLS) == chosen, LEN, base_draw).astype(jnp.int32)


def draw_cache_len(key, part):
    return shared_lengths(key)


def draw_block_pos(key, part):
    lengths = shared_lengths(key)
    block_stretch = jnp.arange(NBLK, dtype=jnp.int32) * BLOCK // STRETCH
    query_stretch = (lengths // STRETCH)[:, None]
    intra_pos = (lengths % STRETCH)[:, None]
    near_pos = jnp.where(block_stretch[None, :] == query_stretch, intra_pos, intra_pos + STRETCH)
    return jnp.where(block_stretch[None, :] >= query_stretch - 1, near_pos, 2 * STRETCH - 1).astype(jnp.int32)


def draw_qkv_bias(key, part):
    bias_draw = 0.5 * jax.random.normal(jax.random.fold_in(key, 31), (QKV,), jnp.float32)
    return jnp.clip(bias_draw, -20.0, 20.0).astype(jnp.bfloat16)


def draw_key_cache(key, part):
    col_total = KVH * HD
    noise_part = jax.random.normal(jax.random.fold_in(key, 41), (ROLLS, NBLK, BLOCK, col_total), jnp.float32)
    region_mean = jax.random.normal(jax.random.fold_in(key, 42), (ROLLS, NBLK, 1, col_total), jnp.float32)
    cached = (noise_part + 0.5 * region_mean).reshape(ROLLS, LEN, col_total)
    return jnp.clip(cached, -16.0, 16.0).astype(jnp.bfloat16)


def draw_value_cache(key, part):
    col_total = KVH * HD
    region_mean = jax.random.normal(jax.random.fold_in(key, 52), (ROLLS, NBLK, 1, col_total), jnp.float32)
    noise_part = jax.random.normal(jax.random.fold_in(key, 51), (ROLLS, NBLK, BLOCK, col_total), jnp.float32)
    cached = noise_part + 2.0 * region_mean
    return jnp.clip(cached.reshape(ROLLS, LEN, col_total), -16.0, 16.0).astype(jnp.bfloat16)


def level_of(key, extent, cuts, smallest, largest):
    gain, own = 1.0, jax.random.fold_in(key, 6)
    for dim, shards_of in cuts:
        steps = jnp.exp(jax.random.uniform(jax.random.fold_in(own, dim), (shards_of,), jnp.float32, smallest / len(cuts), largest / len(cuts)))
        gain = gain * jnp.repeat(steps, extent[dim] // shards_of).reshape([-1 if axis == dim else 1 for axis in range(len(extent))])
    return gain


def centred(rng, dims, deviation, bound, pieces=(), kind=jnp.bfloat16):
    values = jax.random.normal(rng, dims, jnp.float32) * deviation
    if len(pieces) > 0:
        values = level_of(rng, dims, pieces, -0.22, 0.18) * values
    return jnp.clip(values, min=-bound, max=bound).astype(kind)


def setup_inputs(seed: int = 0) -> dict:
    keys = jax.random.split(jax.random.key(seed), 10)
    return {
        "hidden": centred(keys[0], (ROLLS, D), 1.0, 6.0, ((0, 2),)),
        "norm_gain": jnp.clip(1.0 + 0.15 * jax.random.normal(keys[1], (D,), jnp.float32), 0.25, 1.75).astype(jnp.bfloat16),
        "qkv_bias": draw_qkv_bias(jax.random.fold_in(keys[9], 71), 0),
        "qkv_weight": centred(keys[3], (D, QKV), D ** -0.5, 0.09375, ((0, 32),)),
        "out_weight": centred(keys[4], (D, HQ * HD), (HQ * HD) ** -0.5, 0.125, ((0, 32),)),
        "key_cache": draw_key_cache(jax.random.fold_in(keys[9], 71), 0),
        "value_cache": draw_value_cache(jax.random.fold_in(keys[9], 71), 0),
        "cache_len": draw_cache_len(jax.random.fold_in(keys[9], 71), 0),
        "block_pos": draw_block_pos(jax.random.fold_in(keys[9], 71), 0),
    }


rope_base = 10000000.0
norm_eps = 1e-06

def frequencies(width):
    half_width = width // 2
    exact = rope_base ** (-2.0 * np.arange(half_width) / width)
    octave = np.floor(np.log2(exact))
    quantum = 2.0 ** (8.0 - octave)
    return np.floor(exact * quantum) / quantum

def rotate(vectors, positions):
    half_width = vectors.shape[-1] // 2
    inverse = jnp.asarray(frequencies(vectors.shape[-1]), dtype=jnp.float32)
    angles = positions.astype(jnp.float32)[..., None] * inverse
    cosine = jnp.cos(angles)
    sine_part = jnp.sin(angles)
    front_half = vectors[..., :half_width]
    back_half = vectors[..., half_width:]
    return jnp.concatenate([front_half * cosine - back_half * sine_part, back_half * cosine + front_half * sine_part], axis=-1)

def arrange(columns, tp_count):
    lead = columns.shape[:-1]
    per_rank = HQ // tp_count
    query_part = columns[..., :HQ * HD].reshape(lead + (tp_count, per_rank * HD))
    key_part = jnp.repeat(columns[..., HQ * HD:(HQ + KVH) * HD].reshape(lead + (KVH, HD)), tp_count // KVH, axis=-2)
    value_part = jnp.repeat(columns[..., (HQ + KVH) * HD:].reshape(lead + (KVH, HD)), tp_count // KVH, axis=-2)
    return jnp.concatenate([query_part, key_part, value_part], axis=-1)

def reference(hidden, norm_gain, qkv_bias, qkv_weight, out_weight, key_cache, value_cache, cache_len, block_pos):
    group_size = HQ // KVH
    score_scale = HD ** (-0.5)
    hidden_wide = hidden.astype(jnp.float32)
    normed = (hidden_wide * lax.rsqrt(lax.optimization_barrier(jnp.mean(hidden_wide * hidden_wide, axis=1, keepdims=True)) + norm_eps) * norm_gain.astype(jnp.float32)).astype(jnp.bfloat16)
    joint = (jnp.dot(normed, qkv_weight, preferred_element_type=jnp.float32) + qkv_bias.astype(jnp.float32)).astype(jnp.bfloat16)
    queries = joint[:, :HQ * HD].reshape(ROLLS, HQ, HD).astype(jnp.float32)
    new_keys = joint[:, HQ * HD:(HQ + KVH) * HD].reshape(ROLLS, KVH, HD).astype(jnp.float32)
    fresh_value = joint[:, (HQ + KVH) * HD:].reshape(ROLLS, KVH, HD)
    intra_pos = (cache_len % STRETCH).astype(jnp.int32)
    fresh_key = lax.optimization_barrier(rotate(new_keys, jnp.broadcast_to(intra_pos[:, None], (ROLLS, KVH))).astype(jnp.bfloat16))
    self_query = lax.optimization_barrier(rotate(queries, jnp.broadcast_to(intra_pos[:, None], (ROLLS, HQ))).astype(jnp.bfloat16))
    block_query = lax.optimization_barrier(rotate(queries[:, None], jnp.broadcast_to(block_pos[:, :, None], (ROLLS, NBLK, HQ))).astype(jnp.bfloat16))
    self_score = score_scale * jnp.einsum('rkgd,rkd->rkg', self_query.reshape(ROLLS, KVH, group_size, HD).astype(jnp.float32), fresh_key.astype(jnp.float32))

    def one_rollout(per_rollout):
        cached_keys, cached_values, rotated_query, length, own_score, own_value = per_rollout
        keys_wide = cached_keys.reshape(NBLK, BLOCK, KVH, HD).astype(jnp.float32)
        values_wide = cached_values.reshape(NBLK, BLOCK, KVH, HD).astype(jnp.float32)
        query_wide = rotated_query.reshape(NBLK, KVH, group_size, HD).astype(jnp.float32)
        scores = score_scale * jnp.einsum('bkgd,bpkd->kgbp', query_wide, keys_wide)
        valid_mask = jnp.arange(LEN, dtype=jnp.int32).reshape(NBLK, BLOCK) < length
        masked = jnp.where(valid_mask, scores, -jnp.inf)
        top_score = jnp.maximum(lax.optimization_barrier(jnp.max(masked, axis=(2, 3))), own_score)
        weights = jnp.where(valid_mask, jnp.exp(masked - top_score[:, :, None, None]), 0.0)
        own_weight = jnp.exp(own_score - top_score)
        rounded = lax.optimization_barrier(weights.astype(jnp.bfloat16)).astype(jnp.float32)
        own_rounded = lax.optimization_barrier(own_weight.astype(jnp.bfloat16)).astype(jnp.float32)
        numerator = jnp.einsum('kgbp,bpkd->kgd', rounded, values_wide) + own_rounded[:, :, None] * own_value.astype(jnp.float32)[:, None, :]
        denominator = lax.optimization_barrier(jnp.sum(weights, axis=(2, 3))) + own_weight
        return (numerator / denominator[:, :, None]).reshape(HQ * HD).astype(jnp.bfloat16)
    attention = lax.map(one_rollout, (key_cache, value_cache, block_query, cache_len, self_score, fresh_value))
    attended = jnp.dot(attention, out_weight.T, preferred_element_type=jnp.float32).astype(jnp.bfloat16)
    fresh_kv = jnp.concatenate([fresh_key.reshape(ROLLS, KVH * HD), fresh_value.reshape(ROLLS, KVH * HD)], axis=1)
    served_qkv = arrange(qkv_weight, N_TP).reshape(D, N_TP * SCOLS)
    return (attended, fresh_kv, served_qkv, out_weight)
```

```python
import functools

import jax
import jax.numpy as jnp
import numpy as np
from jax import lax
from jax.experimental import pallas as pl
from jax.experimental.pallas import tpu as pltpu
from jax.sharding import PartitionSpec as P

HQ = 16
KVH = 4
HD = 128
GROUP = HQ // KVH
BLOCK = 512
STRETCH = 8192
LANES = 128
SUB = 8

MESH = pl.DeviceIdType.MESH
rope_base = 10000000.0
norm_eps = 1e-06
floor_score = -1e30


def frequencies(width):
    half_width = width // 2
    exact = rope_base ** (-2.0 * np.arange(half_width) / width)
    octave = np.floor(np.log2(exact))
    quantum = 2.0 ** (8.0 - octave)
    return np.floor(exact * quantum) / quantum


def kernel(
    Z, T, X, nr, nb,
    nv_ref, norm_ref, cos_ref, sin_ref, bias_ref, wq_hbm, wo_hbm, k_hbm, v_hbm,
    sq, so, aout_ref, fkv_ref,
    wq, wo, kbuf, vbuf,
    nbuf, pq, qred, qmine, qall, part, pred, attm, att, proj, gat,
    loc_sem, kv_sem, own_sem,
    a_send, a_recv, up_send, dn_send, z_recv, x_send, x_recv,
    n_send, n_recv, d1_send, d1_recv, d2_send, d2_recv, d3_send, d3_recv,
    d4_send, d4_recv, d5_send, d5_recv,
):
    z, tp, x = lax.axis_index("seq"), lax.axis_index("tp"), lax.axis_index("roll")
    ND = Z * T * X
    NG = Z * T
    me = (z * T + tp) * X + x
    gi = z * T + tp
    rows = wq.shape[0]
    per = HQ // T
    QT = (HQ + 2 * KVH)
    NC = nr * KVH

    def coords(i):
        return (lax.div(i, T * X), lax.rem(lax.div(i, X), T), lax.rem(i, X))

    def remote(src, dst, ss, rs, dev):
        return pltpu.make_async_remote_copy(
            src_ref=src, dst_ref=dst, send_sem=ss, recv_sem=rs, device_id=dev, device_id_type=MESH
        )

    lq = pltpu.make_async_copy(wq_hbm, wq, loc_sem.at[0])
    lo = pltpu.make_async_copy(wo_hbm, wo, loc_sem.at[1])
    lk = pltpu.make_async_copy(k_hbm, kbuf, kv_sem.at[0])
    lv = pltpu.make_async_copy(v_hbm, vbuf, kv_sem.at[1])
    lq.start()
    lo.start()
    lk.start()
    lv.start()

    barrier = pltpu.get_barrier_semaphore()

    def greet(i, c):
        other = lax.rem(me + i, ND)
        pl.semaphore_signal(barrier, inc=1, device_id=coords(other), device_id_type=MESH)
        return c

    lax.fori_loop(1, ND, greet, 0)
    pl.semaphore_wait(barrier, ND - 1)

    def norm_copy(dx):
        ox = lax.rem(x + dx, X)
        return remote(norm_ref.at[ox], nbuf.at[x], n_send.at[dx - 1], n_recv.at[x], (z, tp, ox))

    for dx in range(1, X):
        norm_copy(dx).start()

    def pieces(t):
        kv = lax.div(t * KVH, T)
        yield wq.at[:, pl.ds(pl.multiple_of(t * per * HD, LANES), per * HD)], 0, per * HD
        yield wq.at[:, pl.ds(pl.multiple_of((HQ + kv) * HD, LANES), HD)], per * HD, HD
        yield wq.at[:, pl.ds(pl.multiple_of((HQ + KVH + kv) * HD, LANES), HD)], (per + 1) * HD, HD

    def out_piece(t):
        return wo.at[:, pl.ds(pl.multiple_of(t * per * HD, LANES), per * HD)]

    lq.wait()
    lo.wait()
    for dt in list(range(2, T)) + [1]:
        ot = lax.rem(tp + dt, T)
        for src, lo_col, width in pieces(ot):
            remote(src, sq.at[z, tp, x, :, pl.ds(lo_col, width)], a_send.at[dt, 0], a_recv.at[tp, 0], (z, ot, x)).start()
        remote(out_piece(ot), so.at[z, tp, x], a_send.at[dt, 1], a_recv.at[tp, 1], (z, ot, x)).start()
    for src, lo_col, width in pieces(tp):
        pltpu.make_async_copy(src, sq.at[z, tp, x, :, pl.ds(lo_col, width)], own_sem.at[0]).start()
    pltpu.make_async_copy(out_piece(tp), so.at[z, tp, x], own_sem.at[1]).start()

    def wait_local(ref, sem):
        pltpu.make_async_copy(ref, ref, sem).wait()

    both = ((0, sq), (1, so))

    def up(zo, s, j, ref):
        return remote(ref.at[zo, s, x], ref.at[zo, s, x], up_send.at[zo, s, j], z_recv.at[zo, s, j], (z + 1, tp, x))

    def down(zo, s, j, ref):
        return remote(ref.at[zo, s, x], ref.at[zo, s, x], dn_send.at[zo, s, j], z_recv.at[zo, s, j], (z - 1, tp, x))

    def cross(dx, zo, s, j, ref):
        ox = lax.rem(x + dx, X)
        return remote(
            ref.at[zo, s, x], ref.at[zo, s, x], x_send.at[dx - 1, zo, s, j], x_recv.at[x, zo, s, j], (z, tp, ox)
        )

    def spread_own(s):
        for j, ref in both:
            @pl.when(z + 1 < Z)
            def _():
                up(z, s, j, ref).start()

            @pl.when(z > 0)
            def _():
                down(z, s, j, ref).start()

            for dx in range(1, X):
                cross(dx, z, s, j, ref).start()

    def own_piece(dt):
        s = lax.rem(tp + T - dt, T)
        for j, ref in both:
            wait_local(ref.at[z, s, x], a_recv.at[s, j])
        spread_own(s)

    def pass_on(k, i):
        s = lax.rem(tp + i, T)

        @pl.when(z >= k)
        def _():
            for j, ref in both:
                wait_local(ref.at[z - k, s, x], z_recv.at[z - k, s, j])
                for dx in range(1, X):
                    cross(dx, z - k, s, j, ref).start()

                @pl.when(z + 1 < Z)
                def _():
                    up(z - k, s, j, ref).start()

        @pl.when(z + k < Z)
        def _():
            for j, ref in both:
                wait_local(ref.at[z + k, s, x], z_recv.at[z + k, s, j])
                for dx in range(1, X):
                    cross(dx, z + k, s, j, ref).start()

                @pl.when(z > 0)
                def _():
                    down(z + k, s, j, ref).start()

    lhs = norm_ref[x]
    for dx in range(1, X):
        ox = lax.rem(x + dx, X)
        wait_local(nbuf.at[ox], n_recv.at[ox])
        lhs = lhs + nbuf[ox]
    lhs = lhs[:, :rows].astype(jnp.bfloat16)
    for j in range(QT):
        pq[j] = jnp.dot(lhs, wq[:, j * HD:(j + 1) * HD], preferred_element_type=jnp.float32)

    def to_all(count, first, src_of, dst, ss, rs):
        def step(i, c):
            j = lax.rem(first + i, count)

            @pl.when(j != me)
            def _():
                remote(src_of(j), dst, ss, rs, coords(j)).start()

            @pl.when(j == me)
            def _():
                pltpu.make_async_copy(src_of(j), dst, rs).start()

            return c

        lax.fori_loop(0, count, step, 0)

    def drain(count, own, buf, ss):
        @pl.when(own < count)
        def _():
            wait_local(buf.at[pl.ds(0, count - 1)], ss)

        @pl.when(own >= count)
        def _():
            wait_local(buf.at[pl.ds(0, count)], ss)

    to_all(QT, lax.rem(me, QT), lambda j: pq.at[j], qred.at[me], d1_send, d1_recv)
    for j, ref in both:
        wait_local(ref.at[z, tp, x], own_sem.at[j])
    spread_own(tp)

    @pl.when(me < QT)
    def _():
        wait_local(qred, d1_recv)
        total = jnp.sum(qred[...], axis=0) + bias_ref[me]
        qmine[...] = total.astype(jnp.bfloat16).astype(jnp.float32)
        to_all(ND, me, lambda j: qmine, qall.at[me], d2_send, d2_recv)

    for dt in (1, 2):
        if dt < T:
            own_piece(dt)
    wait_local(qall, d2_recv)

    def turn(v, i):
        return v * cos_ref[i:i + 1, :] + pltpu.roll(v, HD // 2, 1) * sin_ref[i:i + 1, :]

    lk.wait()
    lv.wait()
    scale = HD ** (-0.5)
    sub3 = lax.broadcasted_iota(jnp.int32, (QT, SUB, LANES), 1)
    headrow = lax.broadcasted_iota(jnp.int32, (HQ, KVH * HD), 0) // GROUP
    headlane = lax.broadcasted_iota(jnp.int32, (HQ, KVH * HD), 1) // HD
    diag = headrow == headlane
    rowg = lax.broadcasted_iota(jnp.int32, (HQ, HD), 0) // GROUP
    lane = lax.broadcasted_iota(jnp.int32, (HQ, HD), 1)
    pos = lax.broadcasted_iota(jnp.int32, (HQ, BLOCK), 1)
    first_dev = gi == 0
    everything = qall[...]

    def per_head(v):
        out = jnp.zeros((HQ, HD), jnp.float32)
        for g in range(KVH):
            out = jnp.where(rowg == g, v[g:g + 1, :], out)
        return out

    for r in range(nr):
        mine = jnp.sum(jnp.where(sub3 == x * nr + r, everything, 0.0), axis=1)
        q = mine[:HQ]
        fk = turn(mine[HQ:HQ + KVH], r * (nb + 1) + nb).astype(jnp.bfloat16)
        fv = mine[HQ + KVH:]
        fkv_ref[r, :KVH, :] = fk.astype(jnp.float32)
        fkv_ref[r, KVH:, :] = fv
        sqy = turn(q, r * (nb + 1) + nb).astype(jnp.bfloat16).astype(jnp.float32)
        own = scale * jnp.sum(sqy * per_head(fk.astype(jnp.float32)), axis=1, keepdims=True)
        own = jnp.where(first_dev, own, floor_score)
        scores = []
        for b in range(nb):
            bq = turn(q, r * (nb + 1) + b)
            wide = jnp.where(diag, jnp.concatenate([bq] * KVH, axis=1), 0.0).astype(jnp.bfloat16)
            s = scale * lax.dot_general(
                wide, kbuf[r, b * BLOCK:(b + 1) * BLOCK, :], (((1,), (1,)), ((), ())),
                preferred_element_type=jnp.float32,
            )
            scores.append(jnp.where(pos < nv_ref[r * nb + b], s, floor_score))
        top = own
        for s in scores:
            top = jnp.maximum(top, jnp.max(s, axis=1, keepdims=True))
        w_own = jnp.where(first_dev, jnp.exp(own - top), 0.0)
        den = w_own
        acc = jnp.zeros((HQ, KVH * HD), jnp.float32)
        for b in range(nb):
            w = jnp.where(pos < nv_ref[r * nb + b], jnp.exp(scores[b] - top), 0.0)
            den = den + jnp.sum(w, axis=1, keepdims=True)
            acc = acc + jnp.dot(
                w.astype(jnp.bfloat16), vbuf[r, b * BLOCK:(b + 1) * BLOCK, :], preferred_element_type=jnp.float32
            )
        o = w_own.astype(jnp.bfloat16).astype(jnp.float32) * per_head(fv)
        for g in range(KVH):
            o = o + jnp.where(rowg == g, acc[:, g * HD:(g + 1) * HD], 0.0)
        stat = jnp.where(lane < HD // 2, top, den)
        for g in range(KVH):
            part[r * KVH + g] = jnp.concatenate(
                [o[g * GROUP:(g + 1) * GROUP], stat[g * GROUP:(g + 1) * GROUP]], axis=0
            )

    def to_group(i, c):
        j = lax.rem(gi + i, NC)

        @pl.when(j != gi)
        def _():
            remote(part.at[j], pred.at[gi], d3_send, d3_recv, (lax.div(j, T), lax.rem(j, T), x)).start()

        @pl.when(j == gi)
        def _():
            pltpu.make_async_copy(part.at[j], pred.at[gi], d3_recv).start()

        return c

    lax.fori_loop(0, NC, to_group, 0)

    for dt in range(3, T):
        own_piece(dt)

    @pl.when(gi < NC)
    def _():
        wait_local(pred, d3_recv)
        tiles = pred[...]
        o = tiles[:, :GROUP, :]
        m = tiles[:, GROUP:, 0:1]
        l = tiles[:, GROUP:, HD // 2:HD // 2 + 1]
        f = jnp.exp(m - jnp.max(m, axis=0, keepdims=True))
        val = jnp.sum(o * f, axis=0) / jnp.sum(l * f, axis=0)
        val = val.astype(jnp.bfloat16).astype(jnp.float32)
        attm[...] = jnp.concatenate([val, jnp.zeros_like(val)], axis=0)
        to_all(ND, me, lambda j: attm, att.at[x * NC + gi], d4_send, d4_recv)

    for i in range(T):
        pass_on(1, i)
    wait_local(att, d4_recv)

    nrt = nr * X
    prow = lax.broadcasted_iota(jnp.int32, (nrt * SUB, GROUP * HD), 0) % SUB
    plane = lax.broadcasted_iota(jnp.int32, (nrt * SUB, GROUP * HD), 1) // HD
    acc = jnp.zeros((nrt * SUB, rows), jnp.float32)
    for g in range(KVH):
        a = jnp.concatenate([att[i * KVH + g] for i in range(nrt)], axis=0)
        wide = jnp.where(prow == plane, jnp.concatenate([a] * GROUP, axis=1), 0.0).astype(jnp.bfloat16)
        acc = acc + lax.dot_general(
            wide, wo[:, g * GROUP * HD:(g + 1) * GROUP * HD], (((1,), (1,)), ((), ())),
            preferred_element_type=jnp.float32,
        )
    proj[...] = jnp.zeros_like(proj)
    for i in range(nrt):
        proj[i:i + 1, :rows] = jnp.sum(acc[i * SUB:(i + 1) * SUB], axis=0, keepdims=True)
    to_all(ND, me, lambda j: proj, gat.at[me], d5_send, d5_recv)

    for k in range(2, Z):
        for i in range(T):
            pass_on(k, i)

    wait_local(gat, d5_recv)
    aout_ref[...] = gat[...]

    for dx in range(1, X):
        norm_copy(dx).wait_send()
    drain(QT, me, pq, d1_send)

    @pl.when(me < QT)
    def _():
        drain(ND, me, gat, d2_send)

    drain(NC, gi, part, d3_send)

    @pl.when(gi < NC)
    def _():
        drain(ND, me, gat, d4_send)

    drain(ND, me, gat, d5_send)
    for dt in range(1, T):
        for j, ref in both:
            wait_local(ref.at[z, tp, x], a_send.at[dt, j])

    def finish(zs, c):
        zo, s = lax.div(zs, T), lax.rem(zs, T)
        for j, ref in both:
            piece = ref.at[zo, s, x]

            @pl.when((zo <= z) & (z + 1 < Z))
            def _():
                wait_local(piece, up_send.at[zo, s, j])

            @pl.when((zo >= z) & (z > 0))
            def _():
                wait_local(piece, dn_send.at[zo, s, j])

            for dx in range(1, X):
                wait_local(piece, x_send.at[dx - 1, zo, s, j])
                ox = lax.rem(x + dx, X)
                wait_local(ref.at[zo, s, ox], x_recv.at[ox, zo, s, j])
        return c

    lax.fori_loop(0, Z * T, finish, 0)


def make_body(Z, T, X):
    def body(hidden, norm_gain, qkv_bias, qkv_weight, out_weight, key_cache, value_cache, cache_len, block_pos):
        z, tp, x = lax.axis_index("seq"), lax.axis_index("tp"), lax.axis_index("roll")
        nr, D = hidden.shape
        nb = block_pos.shape[1]
        rows = qkv_weight.shape[0]
        per = HQ // T
        SC, HW = (per + 2) * HD, per * HD
        ND, NG, NC, QT = Z * T * X, Z * T, nr * KVH, HQ + 2 * KVH
        wide_rows = hidden.astype(jnp.float32)
        scaled = wide_rows * lax.rsqrt(jnp.mean(wide_rows * wide_rows, axis=1, keepdims=True) + norm_eps)
        normed = (scaled * norm_gain.astype(jnp.float32)).astype(jnp.bfloat16).astype(jnp.float32)
        blocks = lax.dynamic_slice_in_dim(normed, (z * T + tp) * X * rows, X * rows, 1)
        blocks = blocks.reshape(nr, X, rows).transpose(1, 0, 2)
        blocks = jnp.pad(blocks, ((0, 0), (0, 0), (0, LANES - rows)))
        slot = (jnp.arange(X) == x).astype(jnp.float32)
        blocks = (slot[None, :, None, None] * blocks[:, None]).reshape(X, X * nr, LANES)
        intra = cache_len % STRETCH
        pos = jnp.concatenate([block_pos, intra[:, None]], axis=1).reshape(-1)
        ang = pos.astype(jnp.float32)[:, None] * jnp.asarray(frequencies(HD), dtype=jnp.float32)
        cosine, sine = jnp.cos(ang), jnp.sin(ang)
        cos2 = jnp.concatenate([cosine, cosine], axis=1)
        sin2 = jnp.concatenate([-sine, sine], axis=1)
        start = (z * T + tp) * key_cache.shape[1]
        nv = (cache_len[:, None] - start - BLOCK * jnp.arange(nb, dtype=jnp.int32)[None]).reshape(-1)
        bias = qkv_bias.astype(jnp.float32).reshape(QT, 1, HD)
        vm = pl.BlockSpec(memory_space=pltpu.VMEM)
        anys = pl.BlockSpec(memory_space=pl.ANY)
        dma = pltpu.SemaphoreType.DMA
        f32, bf = jnp.float32, jnp.bfloat16
        tile = (SUB, LANES)
        sq, so, gat, fkv = pl.pallas_call(
            functools.partial(kernel, Z, T, X, nr, nb),
            out_shape=(
                jax.ShapeDtypeStruct((Z, T, X, rows, SC), bf),
                jax.ShapeDtypeStruct((Z, T, X, rows, HW), bf),
                jax.ShapeDtypeStruct((ND,) + tile, f32),
                jax.ShapeDtypeStruct((nr, 2 * KVH, HD), f32),
            ),
            in_specs=[pl.BlockSpec(memory_space=pltpu.SMEM)] + [vm] * 4 + [anys] * 4,
            out_specs=(anys, anys, vm, vm),
            scratch_shapes=[
                pltpu.VMEM(qkv_weight.shape, bf),
                pltpu.VMEM(out_weight.shape, bf),
                pltpu.VMEM(key_cache.shape, bf),
                pltpu.VMEM(value_cache.shape, bf),
                pltpu.VMEM((X,) + tile, f32),
                pltpu.VMEM((QT,) + tile, f32),
                pltpu.VMEM((ND,) + tile, f32),
                pltpu.VMEM(tile, f32),
                pltpu.VMEM((QT,) + tile, f32),
                pltpu.VMEM((NC,) + tile, f32),
                pltpu.VMEM((NG,) + tile, f32),
                pltpu.VMEM(tile, f32),
                pltpu.VMEM((X * NC,) + tile, f32),
                pltpu.VMEM(tile, f32),
                pltpu.VMEM((ND,) + tile, f32),
                dma((2,)), dma((2,)), dma((2,)),
                dma((T, 2)), dma((T, 2)),
                dma((Z, T, 2)), dma((Z, T, 2)), dma((Z, T, 2)),
                dma((X - 1, Z, T, 2)), dma((X, Z, T, 2)),
                dma((X - 1,)), dma((X,)),
            ] + [dma] * 10,
            compiler_params=pltpu.CompilerParams(
                collective_id=0, has_side_effects=True, vmem_limit_bytes=48 * 1024 * 1024
            ),
        )(nv, blocks, cos2, sin2, bias, qkv_weight, out_weight, key_cache, value_cache)
        mine = lax.dynamic_slice_in_dim(gat, x * nr, nr, 1)[:, :, :rows]
        attended = mine.transpose(1, 0, 2).reshape(nr, D).astype(bf)
        fresh_kv = fkv.reshape(nr, 2 * KVH * HD).astype(bf)
        return attended, fresh_kv, sq.reshape(D, SC), so.reshape(D, HW)

    return body


def solution(mesh):
    return jax.shard_map(
        make_body(mesh.shape["seq"], mesh.shape["tp"], mesh.shape["roll"]),
        mesh=mesh,
        in_specs=(
            P("roll", None),
            P(),
            P(),
            P(("seq", "tp", "roll"), None),
            P(("seq", "tp", "roll"), None),
            P("roll", ("seq", "tp"), None),
            P("roll", ("seq", "tp"), None),
            P("roll"),
            P("roll", ("seq", "tp")),
        ),
        out_specs=(P("roll", None), P("roll", None), P(None, "tp"), P(None, "tp")),
        check_vma=False,
    )
```

```python
import functools

import jax
import jax.numpy as jnp
import numpy as np
from jax import lax
from jax.experimental import pallas as pl
from jax.experimental.pallas import tpu as pltpu
from jax.sharding import PartitionSpec as P

HQ = 16
KVH = 4
HD = 128
GROUP = HQ // KVH
BLOCK = 512
STRETCH = 8192
LANES = 128
SUB = 8

MESH = pl.DeviceIdType.MESH
rope_base = 10000000.0
norm_eps = 1e-06
floor_score = -1e30


def frequencies(width):
    half_width = width // 2
    exact = rope_base ** (-2.0 * np.arange(half_width) / width)
    octave = np.floor(np.log2(exact))
    quantum = 2.0 ** (8.0 - octave)
    return np.floor(exact * quantum) / quantum


def kernel(
    Z, T, X, nr, nb,
    nv_ref, norm_ref, cos_ref, sin_ref, bias_ref, wq_hbm, wo_hbm, k_hbm, v_hbm,
    sq, so, aout_ref, fkv_ref,
    wq, wo, kbuf, vbuf,
    nbuf, pq, qred, qmine, qall, part, pred, attm, att, proj, gat, fkv,
    loc_sem, kv_sem, own_sem,
    a_send, a_recv, up_send, dn_send, z_recv, x_send, x_recv, twin_send, twin_recv,
    n_send, n_recv, d1_send, d1_recv, d2_send, d2_recv, d3_send, d3_recv,
    d4_send, d4_recv, d5_send, d5_recv,
):
    z, tp, x = lax.axis_index("seq"), lax.axis_index("tp"), lax.axis_index("roll")
    ND = Z * T * X
    NG = Z * T
    me = (z * T + tp) * X + x
    gi = z * T + tp
    rows = wq.shape[0]
    per = HQ // T
    QT = (HQ + 2 * KVH)
    TWINS = (0, T - 1)
    LATE = [i for i in range(T) if i not in TWINS] + list(TWINS)
    NC = nr * KVH

    def coords(i):
        return (lax.div(i, T * X), lax.rem(lax.div(i, X), T), lax.rem(i, X))

    def remote(src, dst, ss, rs, dev):
        return pltpu.make_async_remote_copy(
            src_ref=src, dst_ref=dst, send_sem=ss, recv_sem=rs, device_id=dev, device_id_type=MESH
        )

    lq = pltpu.make_async_copy(wq_hbm, wq, loc_sem.at[0])
    lo = pltpu.make_async_copy(wo_hbm, wo, loc_sem.at[1])
    lk = pltpu.make_async_copy(k_hbm, kbuf, kv_sem.at[0])
    lv = pltpu.make_async_copy(v_hbm, vbuf, kv_sem.at[1])
    lq.start()
    lo.start()
    lk.start()
    lv.start()

    barrier = pltpu.get_barrier_semaphore()

    def greet(i, c):
        other = lax.rem(me + i, ND)
        pl.semaphore_signal(barrier, inc=1, device_id=coords(other), device_id_type=MESH)
        return c

    lax.fori_loop(1, ND, greet, 0)
    pl.semaphore_wait(barrier, ND - 1)

    def norm_copy(dx):
        ox = lax.rem(x + dx, X)
        return remote(norm_ref.at[ox], nbuf.at[x], n_send.at[dx - 1], n_recv.at[x], (z, tp, ox))

    for dx in range(1, X):
        norm_copy(dx).start()

    def pieces(t):
        kv = lax.div(t * KVH, T)
        yield wq.at[:, pl.ds(pl.multiple_of(t * per * HD, LANES), per * HD)], 0, per * HD
        yield wq.at[:, pl.ds(pl.multiple_of((HQ + kv) * HD, LANES), HD)], per * HD, HD
        yield wq.at[:, pl.ds(pl.multiple_of((HQ + KVH + kv) * HD, LANES), HD)], (per + 1) * HD, HD

    def out_piece(t):
        return wo.at[:, pl.ds(pl.multiple_of(t * per * HD, LANES), per * HD)]

    lq.wait()
    lo.wait()
    for dt in list(range(2, T)) + [1]:
        ot = lax.rem(tp + dt, T)
        for src, lo_col, width in pieces(ot):
            remote(src, sq.at[z, tp, x, :, pl.ds(lo_col, width)], a_send.at[dt, 0], a_recv.at[tp, 0], (z, ot, x)).start()
        remote(out_piece(ot), so.at[z, tp, x], a_send.at[dt, 1], a_recv.at[tp, 1], (z, ot, x)).start()
    for src, lo_col, width in pieces(tp):
        pltpu.make_async_copy(src, sq.at[z, tp, x, :, pl.ds(lo_col, width)], own_sem.at[0]).start()
    pltpu.make_async_copy(out_piece(tp), so.at[z, tp, x], own_sem.at[1]).start()

    def wait_local(ref, sem):
        pltpu.make_async_copy(ref, ref, sem).wait()

    both = ((0, sq), (1, so))

    def up(zo, s, j, ref):
        return remote(ref.at[zo, s, x], ref.at[zo, s, x], up_send.at[zo, s, j], z_recv.at[zo, s, j], (z + 1, tp, x))

    def down(zo, s, j, ref):
        return remote(ref.at[zo, s, x], ref.at[zo, s, x], dn_send.at[zo, s, j], z_recv.at[zo, s, j], (z - 1, tp, x))

    def cross(dx, zo, s, j, ref):
        ox = lax.rem(x + dx, X)
        return remote(
            ref.at[zo, s, x], ref.at[zo, s, x], x_send.at[dx - 1, zo, s, j], x_recv.at[x, zo, s, j], (z, tp, ox)
        )

    def spread_own(s):
        for j, ref in both:
            @pl.when(z + 1 < Z)
            def _():
                up(z, s, j, ref).start()

            @pl.when(z > 0)
            def _():
                down(z, s, j, ref).start()

            for dx in range(1, X):
                cross(dx, z, s, j, ref).start()

    def own_piece(dt):
        s = lax.rem(tp + T - dt, T)
        for j, ref in both:
            wait_local(ref.at[z, s, x], a_recv.at[s, j])
        spread_own(s)

    def crosses(zo, i):
        return jnp.logical_not((zo == 0) | (zo == Z - 1)) if i in TWINS else zo >= 0

    def pass_on(k, i):
        s = lax.rem(tp + i, T)

        @pl.when(z >= k)
        def _():
            for j, ref in both:
                wait_local(ref.at[z - k, s, x], z_recv.at[z - k, s, j])

                @pl.when(crosses(z - k, i))
                def _():
                    for dx in range(1, X):
                        cross(dx, z - k, s, j, ref).start()

                @pl.when(z + 1 < Z)
                def _():
                    up(z - k, s, j, ref).start()

        @pl.when(z + k < Z)
        def _():
            for j, ref in both:
                wait_local(ref.at[z + k, s, x], z_recv.at[z + k, s, j])

                @pl.when(crosses(z + k, i))
                def _():
                    for dx in range(1, X):
                        cross(dx, z + k, s, j, ref).start()

                @pl.when(z > 0)
                def _():
                    down(z + k, s, j, ref).start()

    def twin(dx, way, n, j, ref):
        zo = (Z - 1) * way
        piece = ref.at[zo, lax.rem(tp + TWINS[n], T), lax.rem(x + dx, X)]
        nz = z - 1 if way else z + 1
        return remote(piece, piece, twin_send.at[way, dx - 1, n, j], twin_recv.at[way, dx - 1, n, j], (nz, tp, x))

    def each_twin():
        for n in range(len(TWINS)):
            for dx in range(1, X):
                for j, ref in both:
                    yield n, dx, j, ref

    def twin_start():
        for way in (0, 1):
            zo = (Z - 1) * way

            @pl.when(z == zo)
            def _():
                for n, dx, j, ref in each_twin():
                    s, ox = lax.rem(tp + TWINS[n], T), lax.rem(x + dx, X)
                    wait_local(ref.at[zo, s, ox], x_recv.at[ox, zo, s, j])
                    twin(dx, way, n, j, ref).start()

    def twin_pass(k):
        for way in (0, 1):
            zo = (Z - 1) * way

            @pl.when((z + k == zo) if way else (z - k == zo))
            def _():
                for n, dx, j, ref in each_twin():
                    s, ox = lax.rem(tp + TWINS[n], T), lax.rem(x + dx, X)
                    wait_local(ref.at[zo, s, ox], twin_recv.at[way, dx - 1, n, j])
                    if k < Z - 1:
                        twin(dx, way, n, j, ref).start()

    for j, ref in both:
        wait_local(ref.at[z, tp, x], own_sem.at[j])
    spread_own(tp)

    lhs = norm_ref[x]
    for dx in range(1, X):
        ox = lax.rem(x + dx, X)
        wait_local(nbuf.at[ox], n_recv.at[ox])
        lhs = lhs + nbuf[ox]
    lhs = lhs[:, :rows].astype(jnp.bfloat16)
    for j in range(QT):
        pq[j] = jnp.dot(lhs, wq[:, j * HD:(j + 1) * HD], preferred_element_type=jnp.float32)

    def to_all(count, first, src_of, dst, ss, rs):
        def step(i, c):
            j = lax.rem(first + i, count)

            @pl.when(j != me)
            def _():
                remote(src_of(j), dst, ss, rs, coords(j)).start()

            @pl.when(j == me)
            def _():
                pltpu.make_async_copy(src_of(j), dst, rs).start()

            return c

        lax.fori_loop(0, count, step, 0)

    def drain(count, own, buf, ss):
        @pl.when(own < count)
        def _():
            wait_local(buf.at[pl.ds(0, count - 1)], ss)

        @pl.when(own >= count)
        def _():
            wait_local(buf.at[pl.ds(0, count)], ss)

    to_all(QT, lax.rem(me, QT), lambda j: pq.at[j], qred.at[me], d1_send, d1_recv)
    own_piece(1)

    @pl.when(me < QT)
    def _():
        wait_local(qred, d1_recv)
        total = jnp.sum(qred[...], axis=0) + bias_ref[me]
        qmine[...] = total.astype(jnp.bfloat16).astype(jnp.float32)
        to_all(ND, me, lambda j: qmine, qall.at[me], d2_send, d2_recv)

    for dt in range(2, T):
        own_piece(dt)
    wait_local(qall, d2_recv)
    twin_start()

    def turn(v, i):
        return v * cos_ref[i:i + 1, :] + pltpu.roll(v, HD // 2, 1) * sin_ref[i:i + 1, :]

    lk.wait()
    lv.wait()
    scale = HD ** (-0.5)
    sub3 = lax.broadcasted_iota(jnp.int32, (QT, SUB, LANES), 1)
    headrow = lax.broadcasted_iota(jnp.int32, (HQ, KVH * HD), 0) // GROUP
    headlane = lax.broadcasted_iota(jnp.int32, (HQ, KVH * HD), 1) // HD
    diag = headrow == headlane
    rowg = lax.broadcasted_iota(jnp.int32, (HQ, HD), 0) // GROUP
    lane = lax.broadcasted_iota(jnp.int32, (HQ, HD), 1)
    pos = lax.broadcasted_iota(jnp.int32, (HQ, BLOCK), 1)
    first_dev = gi == 0
    everything = qall[...]

    def per_head(v):
        out = jnp.zeros((HQ, HD), jnp.float32)
        for g in range(KVH):
            out = jnp.where(rowg == g, v[g:g + 1, :], out)
        return out

    for r in range(nr):
        if r % 2 == 0 and r // 2 < T:
            pass_on(1, r // 2)
        mine = jnp.sum(jnp.where(sub3 == x * nr + r, everything, 0.0), axis=1)
        q = mine[:HQ]
        fk = turn(mine[HQ:HQ + KVH], r * (nb + 1) + nb).astype(jnp.bfloat16)
        fv = mine[HQ + KVH:]
        for g in range(KVH):
            fkv[r:r + 1, g * HD:(g + 1) * HD] = fk.astype(jnp.float32)[g:g + 1]
            fkv[r:r + 1, (KVH + g) * HD:(KVH + g + 1) * HD] = fv[g:g + 1]
        sqy = turn(q, r * (nb + 1) + nb).astype(jnp.bfloat16).astype(jnp.float32)
        own = scale * jnp.sum(sqy * per_head(fk.astype(jnp.float32)), axis=1, keepdims=True)
        own = jnp.where(first_dev, own, floor_score)
        scores = []
        for b in range(nb):
            bq = turn(q, r * (nb + 1) + b)
            wide = jnp.where(diag, jnp.concatenate([bq] * KVH, axis=1), 0.0).astype(jnp.bfloat16)
            s = scale * lax.dot_general(
                wide, kbuf[r, b * BLOCK:(b + 1) * BLOCK, :], (((1,), (1,)), ((), ())),
                preferred_element_type=jnp.float32,
            )
            scores.append(jnp.where(pos < nv_ref[r * nb + b], s, floor_score))
        top = own
        for s in scores:
            top = jnp.maximum(top, jnp.max(s, axis=1, keepdims=True))
        w_own = jnp.where(first_dev, jnp.exp(own - top), 0.0)
        den = w_own
        acc = jnp.zeros((HQ, KVH * HD), jnp.float32)
        for b in range(nb):
            w = jnp.where(pos < nv_ref[r * nb + b], jnp.exp(scores[b] - top), 0.0)
            den = den + jnp.sum(w, axis=1, keepdims=True)
            acc = acc + jnp.dot(
                w.astype(jnp.bfloat16), vbuf[r, b * BLOCK:(b + 1) * BLOCK, :], preferred_element_type=jnp.float32
            )
        o = w_own.astype(jnp.bfloat16).astype(jnp.float32) * per_head(fv)
        for g in range(KVH):
            o = o + jnp.where(rowg == g, acc[:, g * HD:(g + 1) * HD], 0.0)
        stat = jnp.where(lane < HD // 2, top, den)
        for g in range(KVH):
            part[r * KVH + g] = jnp.concatenate(
                [o[g * GROUP:(g + 1) * GROUP], stat[g * GROUP:(g + 1) * GROUP]], axis=0
            )

    def to_group(i, c):
        j = lax.rem(gi + i, NC)

        @pl.when(j != gi)
        def _():
            remote(part.at[j], pred.at[gi], d3_send, d3_recv, (lax.div(j, T), lax.rem(j, T), x)).start()

        @pl.when(j == gi)
        def _():
            pltpu.make_async_copy(part.at[j], pred.at[gi], d3_recv).start()

        return c

    lax.fori_loop(0, NC, to_group, 0)

    for i in range(min(T, (nr + 1) // 2), T):
        pass_on(1, i)
    twin_pass(1)
    for i in LATE[:T // 2]:
        pass_on(2, i)

    @pl.when(gi < NC)
    def _():
        wait_local(pred, d3_recv)
        tiles = pred[...]
        o = tiles[:, :GROUP, :]
        m = tiles[:, GROUP:, 0:1]
        l = tiles[:, GROUP:, HD // 2:HD // 2 + 1]
        f = jnp.exp(m - jnp.max(m, axis=0, keepdims=True))
        val = jnp.sum(o * f, axis=0) / jnp.sum(l * f, axis=0)
        val = val.astype(jnp.bfloat16).astype(jnp.float32)
        attm[...] = jnp.concatenate([val, jnp.zeros_like(val)], axis=0)
        to_all(ND, me, lambda j: attm, att.at[x * NC + gi], d4_send, d4_recv)

    for i in LATE[T // 2:]:
        pass_on(2, i)
    twin_pass(2)
    wait_local(att, d4_recv)

    nrt = nr * X
    prow = lax.broadcasted_iota(jnp.int32, (nrt * SUB, GROUP * HD), 0) % SUB
    plane = lax.broadcasted_iota(jnp.int32, (nrt * SUB, GROUP * HD), 1) // HD
    acc = jnp.zeros((nrt * SUB, rows), jnp.float32)
    for g in range(KVH):
        a = jnp.concatenate([att[i * KVH + g] for i in range(nrt)], axis=0)
        wide = jnp.where(prow == plane, jnp.concatenate([a] * GROUP, axis=1), 0.0).astype(jnp.bfloat16)
        acc = acc + lax.dot_general(
            wide, wo[:, g * GROUP * HD:(g + 1) * GROUP * HD], (((1,), (1,)), ((), ())),
            preferred_element_type=jnp.float32,
        )
    proj[...] = jnp.zeros_like(proj)
    for i in range(nrt):
        proj[i // nr, i % nr:i % nr + 1, :rows] = jnp.sum(acc[i * SUB:(i + 1) * SUB], axis=0, keepdims=True)
    to_all(ND, me, lambda j: proj.at[lax.rem(j, X)], gat.at[me], d5_send, d5_recv)

    for k in range(3, Z):
        for i in LATE:
            pass_on(k, i)
        twin_pass(k)

    wait_local(gat, d5_recv)
    lane1 = lax.broadcasted_iota(jnp.int32, (SUB, LANES), 1)
    for t in range(ND * rows // LANES):
        row = jnp.zeros((SUB, LANES), jnp.float32)
        for d in range(t * LANES // rows, ((t + 1) * LANES - 1) // rows + 1):
            off = d * rows - t * LANES
            moved = gat[d] if off == 0 else pltpu.roll(gat[d], off % LANES, 1)
            row = jnp.where((lane1 >= off) & (lane1 < off + rows), moved, row)
        aout_ref[:, t * LANES:(t + 1) * LANES] = row[:nr].astype(jnp.bfloat16)
    fkv_ref[...] = fkv[:nr].astype(jnp.bfloat16)

    for dx in range(1, X):
        norm_copy(dx).wait_send()
    drain(QT, me, pq, d1_send)

    @pl.when(me < QT)
    def _():
        drain(ND, me, gat, d2_send)

    drain(NC, gi, part, d3_send)

    @pl.when(gi < NC)
    def _():
        drain(ND, me, gat, d4_send)

    drain(ND, me, gat, d5_send)
    for dt in range(1, T):
        for j, ref in both:
            wait_local(ref.at[z, tp, x], a_send.at[dt, j])

    def finish(zs, c):
        zo, s = lax.div(zs, T), lax.rem(zs, T)
        for j, ref in both:
            piece = ref.at[zo, s, x]

            @pl.when((zo <= z) & (z + 1 < Z))
            def _():
                wait_local(piece, up_send.at[zo, s, j])

            @pl.when((zo >= z) & (z > 0))
            def _():
                wait_local(piece, dn_send.at[zo, s, j])

            i = lax.rem(s - tp + T, T)
            twinned = ((i == TWINS[0]) | (i == TWINS[1])) & ((zo == 0) | (zo == Z - 1))

            @pl.when(jnp.logical_not(twinned) | (zo == z))
            def _():
                for dx in range(1, X):
                    wait_local(piece, x_send.at[dx - 1, zo, s, j])

            @pl.when(jnp.logical_not(twinned))
            def _():
                for dx in range(1, X):
                    ox = lax.rem(x + dx, X)
                    wait_local(ref.at[zo, s, ox], x_recv.at[ox, zo, s, j])

        return c

    lax.fori_loop(0, Z * T, finish, 0)

    for way in (0, 1):
        @pl.when((z > 0) if way else (z + 1 < Z))
        def _():
            for n, dx, j, ref in each_twin():
                wait_local(ref.at[z, tp, x], twin_send.at[way, dx - 1, n, j])


def make_body(Z, T, X):
    def body(hidden, norm_gain, qkv_bias, qkv_weight, out_weight, key_cache, value_cache, cache_len, block_pos):
        z, tp, x = lax.axis_index("seq"), lax.axis_index("tp"), lax.axis_index("roll")
        nr, D = hidden.shape
        nb = block_pos.shape[1]
        rows = qkv_weight.shape[0]
        per = HQ // T
        SC, HW = (per + 2) * HD, per * HD
        ND, NG, NC, QT = Z * T * X, Z * T, nr * KVH, HQ + 2 * KVH
        wide_rows = hidden.astype(jnp.float32)
        scaled = wide_rows * lax.rsqrt(jnp.mean(wide_rows * wide_rows, axis=1, keepdims=True) + norm_eps)
        normed = (scaled * norm_gain.astype(jnp.float32)).astype(jnp.bfloat16).astype(jnp.float32)
        blocks = lax.dynamic_slice_in_dim(normed, (z * T + tp) * X * rows, X * rows, 1)
        blocks = blocks.reshape(nr, X, rows).transpose(1, 0, 2)
        blocks = jnp.pad(blocks, ((0, 0), (0, 0), (0, LANES - rows)))
        slot = (jnp.arange(X) == x).astype(jnp.float32)
        blocks = (slot[None, :, None, None] * blocks[:, None]).reshape(X, X * nr, LANES)
        intra = cache_len % STRETCH
        pos = jnp.concatenate([block_pos, intra[:, None]], axis=1).reshape(-1)
        ang = pos.astype(jnp.float32)[:, None] * jnp.asarray(frequencies(HD), dtype=jnp.float32)
        cosine, sine = jnp.cos(ang), jnp.sin(ang)
        cos2 = jnp.concatenate([cosine, cosine], axis=1)
        sin2 = jnp.concatenate([-sine, sine], axis=1)
        start = (z * T + tp) * key_cache.shape[1]
        nv = (cache_len[:, None] - start - BLOCK * jnp.arange(nb, dtype=jnp.int32)[None]).reshape(-1)
        bias = qkv_bias.astype(jnp.float32).reshape(QT, 1, HD)
        vm = pl.BlockSpec(memory_space=pltpu.VMEM)
        anys = pl.BlockSpec(memory_space=pl.ANY)
        dma = pltpu.SemaphoreType.DMA
        f32, bf = jnp.float32, jnp.bfloat16
        tile = (SUB, LANES)
        sq, so, attended, fresh_kv = pl.pallas_call(
            functools.partial(kernel, Z, T, X, nr, nb),
            out_shape=(
                jax.ShapeDtypeStruct((Z, T, X, rows, SC), bf),
                jax.ShapeDtypeStruct((Z, T, X, rows, HW), bf),
                jax.ShapeDtypeStruct((nr, D), bf),
                jax.ShapeDtypeStruct((nr, 2 * KVH * HD), bf),
            ),
            in_specs=[pl.BlockSpec(memory_space=pltpu.SMEM)] + [vm] * 4 + [pl.BlockSpec(memory_space=pltpu.HBM)] * 4,
            out_specs=(anys, anys, vm, vm),
            scratch_shapes=[
                pltpu.VMEM(qkv_weight.shape, bf),
                pltpu.VMEM(out_weight.shape, bf),
                pltpu.VMEM(key_cache.shape, bf),
                pltpu.VMEM(value_cache.shape, bf),
                pltpu.VMEM((X,) + tile, f32),
                pltpu.VMEM((QT,) + tile, f32),
                pltpu.VMEM((ND,) + tile, f32),
                pltpu.VMEM(tile, f32),
                pltpu.VMEM((QT,) + tile, f32),
                pltpu.VMEM((NC,) + tile, f32),
                pltpu.VMEM((NG,) + tile, f32),
                pltpu.VMEM(tile, f32),
                pltpu.VMEM((X * NC,) + tile, f32),
                pltpu.VMEM((X,) + tile, f32),
                pltpu.VMEM((ND,) + tile, f32),
                pltpu.VMEM((SUB, 2 * KVH * HD), f32),
                dma((2,)), dma((2,)), dma((2,)),
                dma((T, 2)), dma((T, 2)),
                dma((Z, T, 2)), dma((Z, T, 2)), dma((Z, T, 2)),
                dma((X - 1, Z, T, 2)), dma((X, Z, T, 2)),
                dma((2, X - 1, 2, 2)), dma((2, X - 1, 2, 2)),
                dma((X - 1,)), dma((X,)),
            ] + [dma] * 10,
            compiler_params=pltpu.CompilerParams(
                collective_id=0, has_side_effects=True, vmem_limit_bytes=26 * 1024 * 1024
            ),
        )(nv, blocks, cos2, sin2, bias, *(
            pltpu.with_memory_space_constraint(a, pltpu.HBM) for a in (qkv_weight, out_weight, key_cache, value_cache)))
        return attended, fresh_kv, sq.reshape(D, SC), so.reshape(D, HW)

    return body


def solution(mesh):
    return jax.shard_map(
        make_body(mesh.shape["seq"], mesh.shape["tp"], mesh.shape["roll"]),
        mesh=mesh,
        in_specs=(
            P("roll", None),
            P(),
            P(),
            P(("seq", "tp", "roll"), None),
            P(("seq", "tp", "roll"), None),
            P("roll", ("seq", "tp"), None),
            P("roll", ("seq", "tp"), None),
            P("roll"),
            P("roll", ("seq", "tp")),
        ),
        out_specs=(P("roll", None), P("roll", None), P(None, "tp"), P(None, "tp")),
        check_vma=False,
    )
```

```python
import functools

import jax
import jax.numpy as jnp
import numpy as np
from jax import lax
from jax.experimental import pallas as pl
from jax.experimental.pallas import tpu as pltpu
from jax.sharding import PartitionSpec as P

HQ = 16
KVH = 4
HD = 128
GROUP = HQ // KVH
BLOCK = 512
STRETCH = 8192
LANES = 128
SUB = 8

MESH = pl.DeviceIdType.MESH
rope_base = 10000000.0
norm_eps = 1e-06
floor_score = -1e30


def frequencies(width):
    half_width = width // 2
    exact = rope_base ** (-2.0 * np.arange(half_width) / width)
    octave = np.floor(np.log2(exact))
    quantum = 2.0 ** (8.0 - octave)
    return np.floor(exact * quantum) / quantum


def kernel(
    Z, T, X, nr, nb,
    nv_ref, norm_ref, cos_ref, sin_ref, bias_ref, wq_hbm, wo_hbm, k_hbm, v_hbm,
    sq, so, aout_ref, fkv_ref,
    wq, wo, kbuf, vbuf,
    nbuf, pq, qred, qmine, qall, part, pred, attm, att, proj, gat, fkv,
    loc_sem, kv_sem, own_sem,
    a_send, a_recv, up_send, dn_send, z_recv, x_send, x_recv, twin_send, twin_recv,
    n_send, n_recv, d1_send, d1_recv, d2_send, d2_recv, d3_send, d3_recv,
    d4_send, d4_recv, d5_send, d5_recv,
):
    z, tp, x = lax.axis_index("seq"), lax.axis_index("tp"), lax.axis_index("roll")
    ND = Z * T * X
    NG = Z * T
    me = (z * T + tp) * X + x
    gi = z * T + tp
    rows = wq.shape[0]
    per = HQ // T
    QT = (HQ + 2 * KVH)
    TWINS = (0, T - 1)
    LATE = [i for i in range(T) if i not in TWINS] + list(TWINS)
    NC = nr * KVH

    def coords(i):
        return (lax.div(i, T * X), lax.rem(lax.div(i, X), T), lax.rem(i, X))

    def remote(src, dst, ss, rs, dev):
        return pltpu.make_async_remote_copy(
            src_ref=src, dst_ref=dst, send_sem=ss, recv_sem=rs, device_id=dev, device_id_type=MESH
        )

    lq = pltpu.make_async_copy(wq_hbm, wq, loc_sem.at[0])
    lo = pltpu.make_async_copy(wo_hbm, wo, loc_sem.at[1])
    lk = pltpu.make_async_copy(k_hbm, kbuf, kv_sem.at[0])
    lv = pltpu.make_async_copy(v_hbm, vbuf, kv_sem.at[1])
    lq.start()
    lo.start()
    lk.start()
    lv.start()

    barrier = pltpu.get_barrier_semaphore()

    def greet(i, c):
        other = lax.rem(me + i, ND)
        pl.semaphore_signal(barrier, inc=1, device_id=coords(other), device_id_type=MESH)
        return c

    lax.fori_loop(1, ND, greet, 0)
    pl.semaphore_wait(barrier, ND - 1)

    def norm_copy(dx):
        ox = lax.rem(x + dx, X)
        return remote(norm_ref.at[ox], nbuf.at[x], n_send.at[dx - 1], n_recv.at[x], (z, tp, ox))

    for dx in range(1, X):
        norm_copy(dx).start()

    def pieces(t):
        kv = lax.div(t * KVH, T)
        yield wq.at[:, pl.ds(pl.multiple_of(t * per * HD, LANES), per * HD)], 0, per * HD
        yield wq.at[:, pl.ds(pl.multiple_of((HQ + kv) * HD, LANES), HD)], per * HD, HD
        yield wq.at[:, pl.ds(pl.multiple_of((HQ + KVH + kv) * HD, LANES), HD)], (per + 1) * HD, HD

    def out_piece(t):
        return wo.at[:, pl.ds(pl.multiple_of(t * per * HD, LANES), per * HD)]

    lq.wait()
    lo.wait()
    for dt in list(range(2, T)) + [1]:
        ot = lax.rem(tp + dt, T)
        for src, lo_col, width in pieces(ot):
            remote(src, sq.at[z, tp, x, :, pl.ds(lo_col, width)], a_send.at[dt, 0], a_recv.at[tp, 0], (z, ot, x)).start()
        remote(out_piece(ot), so.at[z, tp, x], a_send.at[dt, 1], a_recv.at[tp, 1], (z, ot, x)).start()
    for src, lo_col, width in pieces(tp):
        pltpu.make_async_copy(src, sq.at[z, tp, x, :, pl.ds(lo_col, width)], own_sem.at[0]).start()
    pltpu.make_async_copy(out_piece(tp), so.at[z, tp, x], own_sem.at[1]).start()

    def wait_local(ref, sem):
        pltpu.make_async_copy(ref, ref, sem).wait()

    both = ((0, sq), (1, so))

    def up(zo, s, j, ref):
        return remote(ref.at[zo, s, x], ref.at[zo, s, x], up_send.at[zo, s, j], z_recv.at[zo, s, j], (z + 1, tp, x))

    def down(zo, s, j, ref):
        return remote(ref.at[zo, s, x], ref.at[zo, s, x], dn_send.at[zo, s, j], z_recv.at[zo, s, j], (z - 1, tp, x))

    def cross(dx, zo, s, j, ref):
        ox = lax.rem(x + dx, X)
        return remote(
            ref.at[zo, s, x], ref.at[zo, s, x], x_send.at[dx - 1, zo, s, j], x_recv.at[x, zo, s, j], (z, tp, ox)
        )

    def spread_own(s):
        for j, ref in both:
            @pl.when(z + 1 < Z)
            def _():
                up(z, s, j, ref).start()

            @pl.when(z > 0)
            def _():
                down(z, s, j, ref).start()

            for dx in range(1, X):
                cross(dx, z, s, j, ref).start()

    def own_piece(dt):
        s = lax.rem(tp + T - dt, T)
        for j, ref in both:
            wait_local(ref.at[z, s, x], a_recv.at[s, j])
        spread_own(s)

    def crosses(zo, i):
        return jnp.logical_not((zo == 0) | (zo == Z - 1)) if i in TWINS else zo >= 0

    def pass_on(k, i):
        s = lax.rem(tp + i, T)

        @pl.when(z >= k)
        def _():
            for j, ref in both:
                wait_local(ref.at[z - k, s, x], z_recv.at[z - k, s, j])

                @pl.when(crosses(z - k, i))
                def _():
                    for dx in range(1, X):
                        cross(dx, z - k, s, j, ref).start()

                @pl.when(z + 1 < Z)
                def _():
                    up(z - k, s, j, ref).start()

        @pl.when(z + k < Z)
        def _():
            for j, ref in both:
                wait_local(ref.at[z + k, s, x], z_recv.at[z + k, s, j])

                @pl.when(crosses(z + k, i))
                def _():
                    for dx in range(1, X):
                        cross(dx, z + k, s, j, ref).start()

                @pl.when(z > 0)
                def _():
                    down(z + k, s, j, ref).start()

    def twin(dx, way, n, j, ref):
        zo = (Z - 1) * way
        piece = ref.at[zo, lax.rem(tp + TWINS[n], T), lax.rem(x + dx, X)]
        nz = z - 1 if way else z + 1
        return remote(piece, piece, twin_send.at[way, dx - 1, n, j], twin_recv.at[way, dx - 1, n, j], (nz, tp, x))

    def each_twin():
        for n in range(len(TWINS)):
            for dx in range(1, X):
                for j, ref in both:
                    yield n, dx, j, ref

    def twin_start():
        for way in (0, 1):
            zo = (Z - 1) * way

            @pl.when(z == zo)
            def _():
                for n, dx, j, ref in each_twin():
                    s, ox = lax.rem(tp + TWINS[n], T), lax.rem(x + dx, X)
                    wait_local(ref.at[zo, s, ox], x_recv.at[ox, zo, s, j])
                    twin(dx, way, n, j, ref).start()

    def twin_pass(k):
        for way in (0, 1):
            zo = (Z - 1) * way

            @pl.when((z + k == zo) if way else (z - k == zo))
            def _():
                for n, dx, j, ref in each_twin():
                    s, ox = lax.rem(tp + TWINS[n], T), lax.rem(x + dx, X)
                    wait_local(ref.at[zo, s, ox], twin_recv.at[way, dx - 1, n, j])
                    if k < Z - 1:
                        twin(dx, way, n, j, ref).start()

    for j, ref in both:
        wait_local(ref.at[z, tp, x], own_sem.at[j])
    spread_own(tp)

    lhs = norm_ref[x]
    for dx in range(1, X):
        ox = lax.rem(x + dx, X)
        wait_local(nbuf.at[ox], n_recv.at[ox])
        lhs = lhs + nbuf[ox]
    lhs = lhs[:, :rows].astype(jnp.bfloat16)
    for j in range(QT):
        pq[j] = jnp.dot(lhs, wq[:, j * HD:(j + 1) * HD], preferred_element_type=jnp.float32)

    def to_all(count, first, src_of, dst, ss, rs):
        def step(i, c):
            j = lax.rem(first + i, count)

            @pl.when(j != me)
            def _():
                remote(src_of(j), dst, ss, rs, coords(j)).start()

            @pl.when(j == me)
            def _():
                pltpu.make_async_copy(src_of(j), dst, rs).start()

            return c

        lax.fori_loop(0, count, step, 0)

    def drain(count, own, buf, ss):
        @pl.when(own < count)
        def _():
            wait_local(buf.at[pl.ds(0, count - 1)], ss)

        @pl.when(own >= count)
        def _():
            wait_local(buf.at[pl.ds(0, count)], ss)

    to_all(QT, lax.rem(me, QT), lambda j: pq.at[j], qred.at[me], d1_send, d1_recv)
    own_piece(1)

    @pl.when(me < QT)
    def _():
        wait_local(qred, d1_recv)
        total = jnp.sum(qred[...], axis=0) + bias_ref[:, pl.ds(pl.multiple_of(me * HD, LANES), HD)].astype(jnp.float32)
        qmine[...] = total.astype(jnp.bfloat16).astype(jnp.float32)
        to_all(ND, me, lambda j: qmine, qall.at[me], d2_send, d2_recv)

    for dt in range(2, T):
        own_piece(dt)
    wait_local(qall, d2_recv)
    twin_start()

    def turn(v, i):
        return v * cos_ref[i:i + 1, :] + pltpu.roll(v, HD // 2, 1) * sin_ref[i:i + 1, :]

    lk.wait()
    lv.wait()
    scale = HD ** (-0.5)
    sub3 = lax.broadcasted_iota(jnp.int32, (QT, SUB, LANES), 1)
    headrow = lax.broadcasted_iota(jnp.int32, (HQ, KVH * HD), 0) // GROUP
    headlane = lax.broadcasted_iota(jnp.int32, (HQ, KVH * HD), 1) // HD
    diag = headrow == headlane
    rowg = lax.broadcasted_iota(jnp.int32, (HQ, HD), 0) // GROUP
    lane = lax.broadcasted_iota(jnp.int32, (HQ, HD), 1)
    pos = lax.broadcasted_iota(jnp.int32, (HQ, BLOCK), 1)
    first_dev = gi == 0
    everything = qall[...]

    def per_head(v):
        out = jnp.zeros((HQ, HD), jnp.float32)
        for g in range(KVH):
            out = jnp.where(rowg == g, v[g:g + 1, :], out)
        return out

    for r in range(nr):
        if r % 2 == 0 and r // 2 < T:
            pass_on(1, r // 2)
        mine = jnp.sum(jnp.where(sub3 == x * nr + r, everything, 0.0), axis=1)
        q = mine[:HQ]
        fk = turn(mine[HQ:HQ + KVH], r * (nb + 1) + nb).astype(jnp.bfloat16)
        fv = mine[HQ + KVH:]
        for g in range(KVH):
            fkv[r:r + 1, g * HD:(g + 1) * HD] = fk.astype(jnp.float32)[g:g + 1]
            fkv[r:r + 1, (KVH + g) * HD:(KVH + g + 1) * HD] = fv[g:g + 1]
        sqy = turn(q, r * (nb + 1) + nb).astype(jnp.bfloat16).astype(jnp.float32)
        own = scale * jnp.sum(sqy * per_head(fk.astype(jnp.float32)), axis=1, keepdims=True)
        own = jnp.where(first_dev, own, floor_score)
        scores = []
        for b in range(nb):
            bq = turn(q, r * (nb + 1) + b)
            wide = jnp.where(diag, jnp.concatenate([bq] * KVH, axis=1), 0.0).astype(jnp.bfloat16)
            s = scale * lax.dot_general(
                wide, kbuf[r, b * BLOCK:(b + 1) * BLOCK, :], (((1,), (1,)), ((), ())),
                preferred_element_type=jnp.float32,
            )
            scores.append(jnp.where(pos < nv_ref[r * nb + b], s, floor_score))
        top = own
        for s in scores:
            top = jnp.maximum(top, jnp.max(s, axis=1, keepdims=True))
        w_own = jnp.where(first_dev, jnp.exp(own - top), 0.0)
        den = w_own
        acc = jnp.zeros((HQ, KVH * HD), jnp.float32)
        for b in range(nb):
            w = jnp.where(pos < nv_ref[r * nb + b], jnp.exp(scores[b] - top), 0.0)
            den = den + jnp.sum(w, axis=1, keepdims=True)
            acc = acc + jnp.dot(
                w.astype(jnp.bfloat16), vbuf[r, b * BLOCK:(b + 1) * BLOCK, :], preferred_element_type=jnp.float32
            )
        o = w_own.astype(jnp.bfloat16).astype(jnp.float32) * per_head(fv)
        for g in range(KVH):
            o = o + jnp.where(rowg == g, acc[:, g * HD:(g + 1) * HD], 0.0)
        stat = jnp.where(lane < HD // 2, top, den)
        for g in range(KVH):
            part[r * KVH + g] = jnp.concatenate(
                [o[g * GROUP:(g + 1) * GROUP], stat[g * GROUP:(g + 1) * GROUP]], axis=0
            )

    def to_group(i, c):
        j = lax.rem(gi + i, NC)

        @pl.when(j != gi)
        def _():
            remote(part.at[j], pred.at[gi], d3_send, d3_recv, (lax.div(j, T), lax.rem(j, T), x)).start()

        @pl.when(j == gi)
        def _():
            pltpu.make_async_copy(part.at[j], pred.at[gi], d3_recv).start()

        return c

    lax.fori_loop(0, NC, to_group, 0)

    for i in range(min(T, (nr + 1) // 2), T):
        pass_on(1, i)
    twin_pass(1)
    for i in LATE[:T // 2]:
        pass_on(2, i)

    @pl.when(gi < NC)
    def _():
        wait_local(pred, d3_recv)
        tiles = pred[...]
        o = tiles[:, :GROUP, :]
        m = tiles[:, GROUP:, 0:1]
        l = tiles[:, GROUP:, HD // 2:HD // 2 + 1]
        f = jnp.exp(m - jnp.max(m, axis=0, keepdims=True))
        val = jnp.sum(o * f, axis=0) / jnp.sum(l * f, axis=0)
        val = val.astype(jnp.bfloat16).astype(jnp.float32)
        attm[...] = jnp.concatenate([val, jnp.zeros_like(val)], axis=0)
        to_all(ND, me, lambda j: attm, att.at[x * NC + gi], d4_send, d4_recv)

    for i in LATE[T // 2:]:
        pass_on(2, i)
    twin_pass(2)
    wait_local(att, d4_recv)

    nrt = nr * X
    prow = lax.broadcasted_iota(jnp.int32, (nrt * SUB, GROUP * HD), 0) % SUB
    plane = lax.broadcasted_iota(jnp.int32, (nrt * SUB, GROUP * HD), 1) // HD
    acc = jnp.zeros((nrt * SUB, rows), jnp.float32)
    for g in range(KVH):
        a = jnp.concatenate([att[i * KVH + g] for i in range(nrt)], axis=0)
        wide = jnp.where(prow == plane, jnp.concatenate([a] * GROUP, axis=1), 0.0).astype(jnp.bfloat16)
        acc = acc + lax.dot_general(
            wide, wo[:, g * GROUP * HD:(g + 1) * GROUP * HD], (((1,), (1,)), ((), ())),
            preferred_element_type=jnp.float32,
        )
    proj[...] = jnp.zeros_like(proj)
    for i in range(nrt):
        proj[i // nr, i % nr:i % nr + 1, :rows] = jnp.sum(acc[i * SUB:(i + 1) * SUB], axis=0, keepdims=True)
    to_all(ND, me, lambda j: proj.at[lax.rem(j, X)], gat.at[me], d5_send, d5_recv)

    for k in range(3, Z):
        for i in LATE:
            pass_on(k, i)
        twin_pass(k)

    wait_local(gat, d5_recv)
    lane1 = lax.broadcasted_iota(jnp.int32, (SUB, LANES), 1)
    for t in range(ND * rows // LANES):
        row = jnp.zeros((SUB, LANES), jnp.float32)
        for d in range(t * LANES // rows, ((t + 1) * LANES - 1) // rows + 1):
            off = d * rows - t * LANES
            moved = gat[d] if off == 0 else pltpu.roll(gat[d], off % LANES, 1)
            row = jnp.where((lane1 >= off) & (lane1 < off + rows), moved, row)
        aout_ref[:, t * LANES:(t + 1) * LANES] = row[:nr].astype(jnp.bfloat16)
    fkv_ref[...] = fkv[:nr].astype(jnp.bfloat16)

    for dx in range(1, X):
        norm_copy(dx).wait_send()
    drain(QT, me, pq, d1_send)

    @pl.when(me < QT)
    def _():
        drain(ND, me, gat, d2_send)

    drain(NC, gi, part, d3_send)

    @pl.when(gi < NC)
    def _():
        drain(ND, me, gat, d4_send)

    drain(ND, me, gat, d5_send)
    for dt in range(1, T):
        for j, ref in both:
            wait_local(ref.at[z, tp, x], a_send.at[dt, j])

    def finish(zs, c):
        zo, s = lax.div(zs, T), lax.rem(zs, T)
        for j, ref in both:
            piece = ref.at[zo, s, x]

            @pl.when((zo <= z) & (z + 1 < Z))
            def _():
                wait_local(piece, up_send.at[zo, s, j])

            @pl.when((zo >= z) & (z > 0))
            def _():
                wait_local(piece, dn_send.at[zo, s, j])

            i = lax.rem(s - tp + T, T)
            twinned = ((i == TWINS[0]) | (i == TWINS[1])) & ((zo == 0) | (zo == Z - 1))

            @pl.when(jnp.logical_not(twinned) | (zo == z))
            def _():
                for dx in range(1, X):
                    wait_local(piece, x_send.at[dx - 1, zo, s, j])

            @pl.when(jnp.logical_not(twinned))
            def _():
                for dx in range(1, X):
                    ox = lax.rem(x + dx, X)
                    wait_local(ref.at[zo, s, ox], x_recv.at[ox, zo, s, j])

        return c

    lax.fori_loop(0, Z * T, finish, 0)

    for way in (0, 1):
        @pl.when((z > 0) if way else (z + 1 < Z))
        def _():
            for n, dx, j, ref in each_twin():
                wait_local(ref.at[z, tp, x], twin_send.at[way, dx - 1, n, j])


def make_body(Z, T, X):
    def body(hidden, norm_gain, qkv_bias, qkv_weight, out_weight, key_cache, value_cache, cache_len, block_pos):
        z, tp, x = lax.axis_index("seq"), lax.axis_index("tp"), lax.axis_index("roll")
        nr, D = hidden.shape
        nb = block_pos.shape[1]
        rows = qkv_weight.shape[0]
        per = HQ // T
        SC, HW = (per + 2) * HD, per * HD
        ND, NG, NC, QT = Z * T * X, Z * T, nr * KVH, HQ + 2 * KVH
        wide_rows = hidden.astype(jnp.float32)
        scaled = wide_rows * lax.rsqrt(jnp.mean(wide_rows * wide_rows, axis=1, keepdims=True) + norm_eps)
        normed = (scaled * norm_gain.astype(jnp.float32)).astype(jnp.bfloat16).astype(jnp.float32)
        blocks = lax.dynamic_slice_in_dim(normed, (z * T + tp) * X * rows, X * rows, 1)
        blocks = blocks.reshape(nr, X, rows).transpose(1, 0, 2)
        blocks = jnp.pad(blocks, ((0, 0), (0, 0), (0, LANES - rows)))
        slot = (jnp.arange(X) == x).astype(jnp.float32)
        blocks = (slot[None, :, None, None] * blocks[:, None]).reshape(X, X * nr, LANES)
        intra = cache_len % STRETCH
        pos = jnp.concatenate([block_pos, intra[:, None]], axis=1).reshape(-1)
        ang = pos.astype(jnp.float32)[:, None] * jnp.asarray(frequencies(HD), dtype=jnp.float32)
        cosine, sine = jnp.cos(ang), jnp.sin(ang)
        cos2 = jnp.concatenate([cosine, cosine], axis=1)
        sin2 = jnp.concatenate([-sine, sine], axis=1)
        start = (z * T + tp) * key_cache.shape[1]
        nv = (cache_len[:, None] - start - BLOCK * jnp.arange(nb, dtype=jnp.int32)[None]).reshape(-1)
        bias = qkv_bias.reshape(1, QT * HD)
        vm = pl.BlockSpec(memory_space=pltpu.VMEM)
        anys = pl.BlockSpec(memory_space=pl.ANY)
        dma = pltpu.SemaphoreType.DMA
        f32, bf = jnp.float32, jnp.bfloat16
        tile = (SUB, LANES)
        sq, so, attended, fresh_kv = pl.pallas_call(
            functools.partial(kernel, Z, T, X, nr, nb),
            out_shape=(
                jax.ShapeDtypeStruct((Z, T, X, rows, SC), bf),
                jax.ShapeDtypeStruct((Z, T, X, rows, HW), bf),
                jax.ShapeDtypeStruct((nr, D), bf),
                jax.ShapeDtypeStruct((nr, 2 * KVH * HD), bf),
            ),
            in_specs=[pl.BlockSpec(memory_space=pltpu.SMEM)] + [vm] * 4 + [pl.BlockSpec(memory_space=pltpu.HBM)] * 4,
            out_specs=(anys, anys, vm, vm),
            scratch_shapes=[
                pltpu.VMEM(qkv_weight.shape, bf),
                pltpu.VMEM(out_weight.shape, bf),
                pltpu.VMEM(key_cache.shape, bf),
                pltpu.VMEM(value_cache.shape, bf),
                pltpu.VMEM((X,) + tile, f32),
                pltpu.VMEM((QT,) + tile, f32),
                pltpu.VMEM((ND,) + tile, f32),
                pltpu.VMEM(tile, f32),
                pltpu.VMEM((QT,) + tile, f32),
                pltpu.VMEM((NC,) + tile, f32),
                pltpu.VMEM((NG,) + tile, f32),
                pltpu.VMEM(tile, f32),
                pltpu.VMEM((X * NC,) + tile, f32),
                pltpu.VMEM((X,) + tile, f32),
                pltpu.VMEM((ND,) + tile, f32),
                pltpu.VMEM((SUB, 2 * KVH * HD), f32),
                dma((2,)), dma((2,)), dma((2,)),
                dma((T, 2)), dma((T, 2)),
                dma((Z, T, 2)), dma((Z, T, 2)), dma((Z, T, 2)),
                dma((X - 1, Z, T, 2)), dma((X, Z, T, 2)),
                dma((2, X - 1, 2, 2)), dma((2, X - 1, 2, 2)),
                dma((X - 1,)), dma((X,)),
            ] + [dma] * 10,
            compiler_params=pltpu.CompilerParams(
                collective_id=0, has_side_effects=True, vmem_limit_bytes=26 * 1024 * 1024
            ),
        )(nv, blocks, cos2, sin2, bias, *(
            pltpu.with_memory_space_constraint(a, pltpu.HBM) for a in (qkv_weight, out_weight, key_cache, value_cache)))
        return attended, fresh_kv, sq.reshape(D, SC), so.reshape(D, HW)

    return body


def solution(mesh):
    return jax.shard_map(
        make_body(mesh.shape["seq"], mesh.shape["tp"], mesh.shape["roll"]),
        mesh=mesh,
        in_specs=(
            P("roll", None),
            P(),
            P(),
            P(("seq", "tp", "roll"), None),
            P(("seq", "tp", "roll"), None),
            P("roll", ("seq", "tp"), None),
            P("roll", ("seq", "tp"), None),
            P("roll"),
            P("roll", ("seq", "tp")),
        ),
        out_specs=(P("roll", None), P("roll", None), P(None, "tp"), P(None, "tp")),
        check_vma=False,
    )
```
